32 devices in a mesh: dp: 16 (over z, y, x), mp: 2 (over core).
Axes of the slice: x: 2, y: 2, z: 4, core: 2. Of those that a mesh axis runs over, the one named last changes fastest.
Arguments:
- clean: float32 [64, 3, 4096], P(('dp', 'mp')), may hold values from -1 to 1
- noise: float32 [64, 3, 4096], P(('dp', 'mp')), may hold values from -12 to 12
- lowres: float32 [64, 3, 4096], P(('dp', 'mp')), may hold values from -1 to 1
- aug_noise: float32 [64, 3, 4096], P(('dp', 'mp')), may hold values from -5 to 5
- timesteps: int32 [64], P(('dp', 'mp')), may hold values from 0 to 999
- aug_levels: int32 [64], P(('dp', 'mp')), may hold values from 0 to 999
- lengths: int32 [64], P(('dp', 'mp')), may hold values from 1 to 128
- text: bfloat16 [64, 128, 4096], P(('dp', 'mp')), may hold values from -160 to 160
- w_stem: float32 [6, 128], replicated, may hold values from -2.5 to 2.5
- w_time: float32 [256, 256], replicated, may hold values from -0.375 to 0.375
- conv_one: bfloat16 [1152, 128], replicated, may hold values from -0.1875 to 0.1875
- conv_two: bfloat16 [1152, 128], replicated, may hold values from -0.1875 to 0.1875
- kv_weight: bfloat16 [4096, 256], P('mp'), may hold values from -0.09375 to 0.09375
- w_query: bfloat16 [128, 128], replicated, may hold values from -0.5 to 0.5
- w_output: bfloat16 [128, 128], replicated, may hold values from -0.5 to 0.5
- w_head: bfloat16 [3, 128], replicated, may hold values from -0.5 to 0.5
Outputs:
- conv_one_update: float32 [1152, 128], P(('dp', 'mp'))
- conv_two_update: float32 [1152, 128], P(('dp', 'mp'))
- kv_update: float32 [4096, 256], P('mp', 'dp')
- loss_mean: float32 [], replicated
The draws below stay inside these ranges and needn't reach their ends.
All inputs are finite; a program needn't handle non-finite values.
Results may differ from the reference program's by a relative error of at most 0.03.
The reference program's roundings to bfloat16 on the way count: a program that leaves them out, or rounds other values in their place, can miss the bound.
Values may be sent and summed in bfloat16 or wider, within the bound.
No kernel may reach another device: no remote copies, remote signals or barrier semaphores. Data moves between devices by JAX's collectives and lax.ppermute only.
A program may use at most 128 MiB of HBM per device.

```python
import math
import jax
import jax.numpy as jnp
from jax import lax

S = 64
C = 128
GROUPS = 32
HEADS = 2
HEAD_DIM = 64
A = 128
L = 128
DT = 4096
FREQS = 64
STEPS = 1000
BATCH = 64


def draw_text(key, part):
    base = jax.random.normal(jax.random.fold_in(key, 11), (BATCH, L, DT), jnp.float32)
    base = jnp.clip(base, -4.0, 4.0)
    return base.astype(jnp.bfloat16)


def draw_noise(key, part):
    ramp = jnp.arange(BATCH, dtype=jnp.float32) / max(BATCH - 1, 1)
    spread = (1.0 + 2.0 * ramp)[:, None, None]
    base = jnp.clip(jax.random.normal(jax.random.fold_in(key, 22), (BATCH, 3, S * S), jnp.float32), -4.0, 4.0)
    return (base * spread).astype(jnp.float32)


def set_ends(entries, stream_key, least, high):
    longest = entries.shape.index(max(entries.shape))
    spots = []
    for shift in (0, 1):
        where = [jax.random.randint(jax.random.fold_in(stream_key, axis), (), 0, length) for axis, length in enumerate(entries.shape)]
        where[longest] = (where[longest] + shift) % entries.shape[longest]
        spots.append(tuple(where))
    return entries.at[spots[0]].set(least).at[spots[1]].set(high)


def steps_of(rng, extent, cuts, low, largest):
    def one(axis_at, shards_of):
        steps = jax.random.uniform(jax.random.fold_in(jax.random.fold_in(rng, 6), axis_at), (shards_of,), jnp.float32, low / len(cuts), largest / len(cuts))
        return jnp.repeat(jnp.exp(steps), extent[axis_at] // shards_of).reshape((-1,) + (1,) * (len(extent) - axis_at - 1))

    gain = one(*cuts[0])
    for cut in cuts[1:]:
        gain = gain * one(*cut)
    return gain


def gaussian(stream_key, extent, scale, limit, cuts=(), kind=jnp.bfloat16):
    values = scale * jax.random.normal(stream_key, extent, jnp.float32)
    if cuts:
        values = values * steps_of(stream_key, extent, cuts, -0.22, 0.18)
    return jnp.clip(values, -limit, limit).astype(kind)


def setup_inputs(seed: int = 0) -> dict:
    arg_keys = jax.random.split(jax.random.key(seed), 17)
    clean = jnp.clip(jax.random.uniform(arg_keys[0], (BATCH, 3, S * S), jnp.float32, -1.0, 1.0) * steps_of(arg_keys[0], (BATCH, 3, S * S), ((0, 32),), -0.4, 0.0), -1.0, 1.0)
    noise = draw_noise(jax.random.fold_in(arg_keys[16], 71), 0)
    lowres = jnp.clip(jax.random.uniform(arg_keys[2], (BATCH, 3, S * S), jnp.float32, -1.0, 1.0) * steps_of(arg_keys[2], (BATCH, 3, S * S), ((0, 32),), -0.4, 0.0), -1.0, 1.0)
    aug_noise = gaussian(arg_keys[3], (BATCH, 3, S * S), 1.0, 5.0, ((0, 32),), jnp.float32)
    timesteps = set_ends(jax.random.randint(arg_keys[4], (BATCH,), 0, STEPS), jax.random.fold_in(arg_keys[4], 1), 0, STEPS - 1).astype(jnp.int32)
    aug_levels = set_ends(jax.random.randint(arg_keys[5], (BATCH,), 0, STEPS), jax.random.fold_in(arg_keys[5], 1), 0, STEPS - 1).astype(jnp.int32)
    lengths = set_ends(jax.random.randint(arg_keys[6], (BATCH,), 1, L + 1), jax.random.fold_in(arg_keys[6], 1), 1, L).astype(jnp.int32)
    text = draw_text(jax.random.fold_in(arg_keys[16], 71), 0)
    w_stem = gaussian(arg_keys[8], (6, C), 6 ** -0.5, 2.5, (), jnp.float32)
    w_time = gaussian(arg_keys[9], (4 * FREQS, 2 * C), (4 * FREQS) ** -0.5, 0.375, (), jnp.float32)
    conv_one = gaussian(arg_keys[10], (9 * C, C), (9 * C) ** -0.5, 0.1875)
    conv_two = gaussian(arg_keys[11], (9 * C, C), (9 * C) ** -0.5, 0.1875)
    kv_weight = gaussian(arg_keys[12], (DT, 2 * A), DT ** -0.5, 0.09375, ((0, 2),))
    w_query = gaussian(arg_keys[13], (C, A), C ** -0.5, 0.5)
    w_output = gaussian(arg_keys[14], (A, C), A ** -0.5, 0.5)
    w_head = gaussian(arg_keys[15], (3, C), C ** -0.5, 0.5)
    return dict(clean=clean, noise=noise, lowres=lowres, aug_noise=aug_noise, timesteps=timesteps, aug_levels=aug_levels, lengths=lengths, text=text, w_stem=w_stem, w_time=w_time, conv_one=conv_one, conv_two=conv_two, kv_weight=kv_weight, w_query=w_query, w_output=w_output, w_head=w_head)


def signal_level(index):
    ratio = (index.astype(jnp.float32) / STEPS + 0.008) / 1.008
    cosine = jnp.cos(ratio * (math.pi / 2.0))
    return cosine * cosine

def sinusoid(index):
    freqs = jnp.exp(-math.log(10000.0) * jnp.arange(FREQS, dtype=jnp.float32) / FREQS)
    angles = index.astype(jnp.float32) * freqs
    return jnp.concatenate([jnp.sin(angles), jnp.cos(angles)])

def prepare(clean, noise, lowres, aug_noise, tstep, level, w_stem, w_time):
    signal = signal_level(tstep)
    aug_signal = signal_level(level)
    noisy = jnp.sqrt(signal) * clean + jnp.sqrt(1.0 - signal) * noise
    low_noisy = jnp.sqrt(aug_signal) * lowres + jnp.sqrt(1.0 - aug_signal) * aug_noise
    stacked = jnp.concatenate([noisy, low_noisy], axis=0)
    h_start = jnp.einsum('kp,kc->pc', stacked, w_stem, precision=lax.Precision.HIGHEST)
    feature = jnp.concatenate([sinusoid(tstep), sinusoid(level)])[None, :]
    embed = jax.nn.silu(jnp.dot(feature, w_time, precision=lax.Precision.HIGHEST))[0]
    channels = w_stem.shape[1]
    return (h_start, embed[:channels], embed[channels:])

def group_matrix(channels):
    members = channels // GROUPS
    labels = jnp.arange(channels) // members
    return (labels[:, None] == labels[None, :]).astype(jnp.float32) / members

def group_norm(values, grouping):
    average = jnp.dot(lax.optimization_barrier(jnp.mean(values, axis=0, keepdims=True)), grouping, precision=lax.Precision.HIGHEST)
    centred = values - average
    spread = jnp.dot(lax.optimization_barrier(jnp.mean(centred * centred, axis=0, keepdims=True)), grouping, precision=lax.Precision.HIGHEST)
    return centred * lax.rsqrt(spread + 1e-05)

def convolve(activation, weight):
    channels = weight.shape[1]
    kernel = weight.reshape(3, 3, channels, channels)
    picture = activation.reshape(1, S, S, channels)
    result = lax.conv_general_dilated(picture, kernel, (1, 1), 'SAME', dimension_numbers=('NHWC', 'HWIO', 'NHWC'), preferred_element_type=jnp.float32)
    return result.reshape(S * S, channels)

def image_loss(conv_one, conv_two, keys_values, h_start, scale, shift, keep, w_query, w_output, w_head, noise):
    channels = conv_one.shape[1]
    grouping = group_matrix(channels)
    act_one = jax.nn.silu(group_norm(h_start, grouping)).astype(jnp.bfloat16)
    conv_out_one = convolve(act_one, conv_one)
    act_two = jax.nn.silu(group_norm(conv_out_one, grouping) * (1.0 + scale) + shift).astype(jnp.bfloat16)
    h_mid = h_start + convolve(act_two, conv_two)
    normed = group_norm(h_mid, grouping).astype(jnp.bfloat16)
    queries = (jnp.dot(normed, w_query, preferred_element_type=jnp.float32) * HEAD_DIM ** (-0.5)).astype(jnp.bfloat16)
    width = w_query.shape[1]
    pieces = []
    for head_index in range(HEADS):
        lower = head_index * HEAD_DIM
        upper = lower + HEAD_DIM
        scores = jnp.dot(queries[:, lower:upper], keys_values[:, lower:upper].T, preferred_element_type=jnp.float32)
        scores = jnp.where(keep[None, :], scores, -1e+30)
        highest = lax.optimization_barrier(jnp.max(scores, axis=1, keepdims=True))
        weights = jnp.exp(scores - highest)
        probs = (weights / lax.optimization_barrier(jnp.sum(weights, axis=1, keepdims=True))).astype(jnp.bfloat16)
        pieces.append(jnp.dot(probs, keys_values[:, width + lower:width + upper], preferred_element_type=jnp.float32))
    attended = jnp.concatenate(pieces, axis=1).astype(jnp.bfloat16)
    h_out = h_mid + jnp.dot(attended, w_output, preferred_element_type=jnp.float32)
    pred = jnp.einsum('kc,pc->kp', w_head.astype(jnp.float32), h_out.astype(jnp.bfloat16).astype(jnp.float32))
    error = pred - noise
    return jnp.sum(error * error)

def normalize(grad):
    return grad * lax.rsqrt(jnp.mean(grad * grad) + 1e-06)

def reference(clean, noise, lowres, aug_noise, timesteps, aug_levels, lengths, text, w_stem, w_time, conv_one, conv_two, kv_weight, w_query, w_output, w_head):

    def visit(carry, items):
        grad_one, grad_two, grad_kv, total = carry
        clean_i, noise_i, low_i, aug_i, tstep, level, length, text_i = items
        h_start, scale, shift = prepare(clean_i, noise_i, low_i, aug_i, tstep, level, w_stem, w_time)
        keys_values = jnp.dot(text_i, kv_weight, preferred_element_type=jnp.float32).astype(jnp.bfloat16)
        keep = jnp.arange(text_i.shape[0]).astype(jnp.int32) < length
        value, pullback = jax.vjp(lambda first, second, third: image_loss(first, second, third, h_start, scale, shift, keep, w_query, w_output, w_head, noise_i), conv_one, conv_two, keys_values)
        part_one, part_two, part_kv = pullback(jnp.ones((), value.dtype))
        grad_kv = grad_kv + jnp.dot(text_i.T, part_kv, preferred_element_type=jnp.float32)
        return ((grad_one + part_one.astype(jnp.float32), grad_two + part_two.astype(jnp.float32), grad_kv, total + value), None)
    start = (jnp.zeros(conv_one.shape, jnp.float32), jnp.zeros(conv_two.shape, jnp.float32), jnp.zeros(kv_weight.shape, jnp.float32), jnp.zeros((), jnp.float32))
    finals, unused = lax.scan(visit, start, (clean, noise, lowres, aug_noise, timesteps, aug_levels, lengths, text))
    grad_one, grad_two, grad_kv, total = finals
    count = clean.shape[0] * clean.shape[1] * clean.shape[2]
    return (normalize(grad_one), normalize(grad_two), normalize(grad_kv), total / count)
```

```python
import math

import jax
import jax.numpy as jnp
from jax import lax
from jax.sharding import PartitionSpec as P

S = 64
GROUPS = 32
HEADS = 2
HEAD_DIM = 64
FREQS = 64
STEPS = 1000


def signal_level(index):
    ratio = (index.astype(jnp.float32) / STEPS + 0.008) / 1.008
    cosine = jnp.cos(ratio * (math.pi / 2.0))
    return cosine * cosine


def sinusoid(index):
    freqs = jnp.exp(-math.log(10000.0) * jnp.arange(FREQS, dtype=jnp.float32) / FREQS)
    angles = index.astype(jnp.float32) * freqs
    return jnp.concatenate([jnp.sin(angles), jnp.cos(angles)])


def prepare(clean, noise, lowres, aug_noise, tstep, level, w_stem, w_time):
    signal = signal_level(tstep)
    aug_signal = signal_level(level)
    noisy = jnp.sqrt(signal) * clean + jnp.sqrt(1.0 - signal) * noise
    low_noisy = jnp.sqrt(aug_signal) * lowres + jnp.sqrt(1.0 - aug_signal) * aug_noise
    stacked = jnp.concatenate([noisy, low_noisy], axis=0)
    h_start = jnp.einsum("kp,kc->pc", stacked, w_stem, precision=lax.Precision.HIGHEST)
    feature = jnp.concatenate([sinusoid(tstep), sinusoid(level)])[None, :]
    embed = jax.nn.silu(jnp.dot(feature, w_time, precision=lax.Precision.HIGHEST))[0]
    channels = w_stem.shape[1]
    return (h_start, embed[:channels], embed[channels:])


def group_matrix(channels):
    members = channels // GROUPS
    labels = jnp.arange(channels) // members
    return (labels[:, None] == labels[None, :]).astype(jnp.float32) / members


def group_norm(values, grouping):
    average = jnp.dot(
        jnp.mean(values, axis=0, keepdims=True), grouping, precision=lax.Precision.HIGHEST
    )
    centred = values - average
    spread = jnp.dot(
        jnp.mean(centred * centred, axis=0, keepdims=True),
        grouping,
        precision=lax.Precision.HIGHEST,
    )
    return centred * lax.rsqrt(spread + 1e-05)


def convolve(activation, weight):
    channels = weight.shape[1]
    kernel = weight.reshape(3, 3, channels, channels)
    picture = activation.reshape(1, S, S, channels)
    result = lax.conv_general_dilated(
        picture,
        kernel,
        (1, 1),
        "SAME",
        dimension_numbers=("NHWC", "HWIO", "NHWC"),
        preferred_element_type=jnp.float32,
    )
    return result.reshape(S * S, channels)


def conv_stage(conv_one, conv_two, h_start, scale, shift):
    channels = conv_one.shape[1]
    grouping = group_matrix(channels)
    act_one = jax.nn.silu(group_norm(h_start, grouping)).astype(jnp.bfloat16)
    conv_out_one = convolve(act_one, conv_one)
    act_two = jax.nn.silu(group_norm(conv_out_one, grouping) * (1.0 + scale) + shift).astype(
        jnp.bfloat16
    )
    return h_start + convolve(act_two, conv_two)


def attention_stage(h_mid, keys_values, keep, w_query, w_output, w_head, noise):
    channels = h_mid.shape[1]
    grouping = group_matrix(channels)
    normed = group_norm(h_mid, grouping).astype(jnp.bfloat16)
    queries = (
        jnp.dot(normed, w_query, preferred_element_type=jnp.float32) * HEAD_DIM ** (-0.5)
    ).astype(jnp.bfloat16)
    width = w_query.shape[1]
    pieces = []
    for head_index in range(HEADS):
        lower = head_index * HEAD_DIM
        upper = lower + HEAD_DIM
        scores = jnp.dot(
            queries[:, lower:upper],
            keys_values[:, lower:upper].T,
            preferred_element_type=jnp.float32,
        )
        scores = jnp.where(keep[None, :], scores, -1e30)
        highest = jnp.max(scores, axis=1, keepdims=True)
        weights = jnp.exp(scores - highest)
        probs = (weights / jnp.sum(weights, axis=1, keepdims=True)).astype(jnp.bfloat16)
        pieces.append(
            jnp.dot(
                probs,
                keys_values[:, width + lower : width + upper],
                preferred_element_type=jnp.float32,
            )
        )
    attended = jnp.concatenate(pieces, axis=1).astype(jnp.bfloat16)
    h_out = h_mid + jnp.dot(attended, w_output, preferred_element_type=jnp.float32)
    pred = jnp.einsum(
        "kc,pc->kp", w_head, h_out.astype(jnp.bfloat16), preferred_element_type=jnp.float32
    )
    error = pred - noise
    return jnp.sum(error * error)


def local(
    clean,
    noise,
    lowres,
    aug_noise,
    timesteps,
    aug_levels,
    lengths,
    text,
    w_stem,
    w_time,
    conv_one,
    conv_two,
    kv_weight,
    w_query,
    w_output,
    w_head,
):
    images = clean.shape[0]
    tokens = text.shape[1]
    features = text.shape[2]
    width = kv_weight.shape[1]
    half = kv_weight.shape[0]
    ranks = lax.axis_size("mp")
    mine = lax.axis_index("mp")
    everyone = ("dp", "mp")
    flat_text = text.reshape(images * tokens, features)

    def hop(value, shift):
        return lax.ppermute(value, "mp", [(at, (at + shift) % ranks) for at in range(ranks)])

    def columns(owner):
        return lax.dynamic_slice_in_dim(flat_text, owner * half, half, axis=1)

    text_parts = [columns(mine)]
    for shift in range(1, ranks):
        text_parts.append(hop(columns((mine + shift) % ranks), shift))
    piece = lax.all_gather(kv_weight, "mp", axis=0, tiled=True)
    flat = jnp.dot(flat_text, piece, preferred_element_type=jnp.float32)
    keys_values = flat.reshape(images, tokens, width).astype(jnp.bfloat16)
    mids, conv_backs = [], []
    for at in range(images):
        h_start, scale, shift_by = prepare(
            clean[at], noise[at], lowres[at], aug_noise[at], timesteps[at], aug_levels[at], w_stem, w_time
        )
        h_mid, back = jax.vjp(
            lambda first, second: conv_stage(first, second, h_start, scale, shift_by),
            conv_one,
            conv_two,
        )
        mids.append(h_mid)
        conv_backs.append(back)
    mid_cots, kv_cots, local_loss = [], [], 0.0
    for at in range(images):
        keep = jnp.arange(tokens) < lengths[at]
        value, back = jax.vjp(
            lambda mid, pairs: attention_stage(
                mid, pairs, keep, w_query, w_output, w_head, noise[at]
            ),
            mids[at],
            keys_values[at],
        )
        mid_cot, kv_cot = back(jnp.ones((), jnp.float32))
        mid_cots.append(mid_cot)
        kv_cots.append(kv_cot)
        local_loss = local_loss + value
    cot = jnp.concatenate(kv_cots, axis=0)
    row_share = jnp.zeros((width, half), jnp.float32)
    for shift in range(ranks):
        row_share = row_share + lax.dot_general(
            cot if shift == 0 else hop(cot, shift),
            text_parts[shift],
            (((0,), (0,)), ((), ())),
            preferred_element_type=jnp.float32,
        )
    row_share, mid_cots = lax.optimization_barrier((row_share, mid_cots))
    devices = lax.axis_size(everyone)

    def scatter_sum(value, axes):
        pieces = value.astype(jnp.bfloat16).reshape(
            lax.axis_size(axes), value.shape[0] // lax.axis_size(axes), value.shape[1]
        )
        swapped = lax.all_to_all(pieces, axes, split_axis=0, concat_axis=0, tiled=True)
        return jnp.sum(swapped.astype(jnp.float32), axis=0)

    grad_kv = scatter_sum(row_share, "dp")
    parts = [back(mid_cot) for back, mid_cot in zip(conv_backs, mid_cots)]
    channels = conv_one.shape[1]
    local_two = sum(part[1].astype(jnp.float32) for part in parts)
    local_two, grad_kv = lax.optimization_barrier((local_two, grad_kv))
    grad_two = scatter_sum(local_two, everyone)
    grad_one = scatter_sum(sum(part[0].astype(jnp.float32) for part in parts), everyone)
    square_one = jnp.sum(grad_one * grad_one)
    square_two = jnp.sum(grad_two * grad_two)
    square_kv = jnp.sum(grad_kv * grad_kv)
    sums = jnp.stack([square_one, square_two, square_kv, local_loss])
    sums = jnp.pad(sums, (0, channels - sums.shape[0]))
    copies = jnp.broadcast_to(sums[None, None, :], (devices, 8, channels))
    copies = lax.all_to_all(copies, everyone, split_axis=0, concat_axis=0, tiled=True)
    totals = jnp.sum(copies[:, 0, :], axis=0)
    total_one, total_two, total_kv, loss_total = totals[0], totals[1], totals[2], totals[3]
    conv_count = conv_one.shape[0] * channels
    kv_count = half * ranks * width
    conv_one_update = grad_one * lax.rsqrt(total_one / conv_count + 1e-06)
    conv_two_update = grad_two * lax.rsqrt(total_two / conv_count + 1e-06)
    kv_update = (grad_kv * lax.rsqrt(total_kv / kv_count + 1e-06)).T
    loss_mean = loss_total / (images * devices * clean.shape[1] * clean.shape[2])
    return (conv_one_update, conv_two_update, kv_update, loss_mean)


def solution(mesh):
    return jax.shard_map(
        local,
        mesh=mesh,
        in_specs=(
            P(("dp", "mp"), None, None),
            P(("dp", "mp"), None, None),
            P(("dp", "mp"), None, None),
            P(("dp", "mp"), None, None),
            P(("dp", "mp")),
            P(("dp", "mp")),
            P(("dp", "mp")),
            P(("dp", "mp"), None, None),
            P(),
            P(),
            P(),
            P(),
            P("mp", None),
            P(),
            P(),
            P(),
        ),
        out_specs=(P(("dp", "mp"), None), P(("dp", "mp"), None), P("mp", "dp"), P()),
        check_vma=False,
    )
```
